32 devices in a mesh: sub: 8 (over z, y), grp: 4 (over x, core).
Axes of the slice: x: 2, y: 2, z: 4, core: 2. Of those that a mesh axis runs over, the one named last changes fastest.
Arguments:
- rr_inverse: float32 [64, 512, 512], P(('sub', 'grp')), may hold values from -4 to 4, as said below
- corner_modes: float32 [64, 64, 512], P(('sub', 'grp')), may hold values from -0.5 to 0.5
- coarse_inverse: float32 [2048, 2048], P(('sub', 'grp')), may hold values from -1 to 1, as said below
- inertia: float32 [64, 512], P(('sub', 'grp')), may hold values from 0.5 to 2
- disp_now: float32 [8, 64, 512], P(None, ('sub', 'grp')), may hold values from -4 to 4
- vel_now: float32 [8, 64, 512], P(None, ('sub', 'grp')), may hold values from -4 to 4
- acc_now: float32 [8, 64, 512], P(None, ('sub', 'grp')), may hold values from -8 to 8
- load_next: float32 [8, 64, 512], P(None, ('sub', 'grp')), may hold values from -10 to 10
- basis_rows: float32 [32768, 256], P(('sub', 'grp')), may hold values from -0.03125 to 0.03125
- piece_owner: int32 [32], replicated, may hold values from 0 to 31, each once
Outputs:
- disp_new: float32 [8, 64, 512], P(None, ('sub', 'grp'))
- vel_new: float32 [8, 64, 512], P(None, ('sub', 'grp'))
- projection: float32 [256, 8], replicated
- r_factor: float32 [8, 8], replicated
- new_columns: float32 [8, 32768], P(None, ('sub', 'grp'))
The draws below stay inside these ranges and needn't reach their ends.
Inputs may be any that keep to these rules, and one draw needn't show every extreme that they name: piece_owner is a permutation. `rr_inverse`: each of the 64 blocks is symmetric positive definite. `coarse_inverse`: symmetric positive definite.
All inputs are finite; a program needn't handle non-finite values.
Results may differ from the reference program's by a relative error of at most 0.00018.
Values sent between devices are 32-bit elements; how exact they have to be, the bound alone decides.
A program may use at most 64 MiB of HBM per device.

```python
import math
import jax
import jax.numpy as jnp
from jax import lax

NR = 512
NC = 32
RANK = 256
NCASE = 8
ITERS = 2
NI = 128
SUBDOMAINS = 64
NCG = 2048
NROWS = 32768
PIECES = 32


def coupled_block(key, order, floor_value, ceiling_value, shared):
    key_noise, key_diag = jax.random.split(key)
    noise = jax.random.uniform(key_noise, (order, order), jnp.float32, -1.0, 1.0)
    upper = jnp.triu(noise, 1)
    coupling = (upper + upper.T) * (0.3 * math.sqrt(3.0) / math.sqrt(order))
    logs = jax.random.uniform(key_diag, (order,), jnp.float32, math.log(floor_value), math.log(ceiling_value))
    roots = jnp.exp(0.5 * logs)
    middle = jnp.eye(order, dtype=jnp.float32) + coupling + shared / order
    return roots[:, None] * middle * roots[None, :]


def draw_rr_inverse(key, part):
    subkeys = jax.random.split(key, SUBDOMAINS)
    return lax.map(lambda single: coupled_block(single, NR, 0.05, 2.0, 0.0), subkeys)


def draw_coarse_inverse(key, part):
    return coupled_block(key, NCG, 0.1, 0.5, 0.3)


def draw_load_next(key, part):
    key_base, key_rows = jax.random.split(key, 2)
    position = jnp.arange(SUBDOMAINS, dtype=jnp.float32) / max(SUBDOMAINS - 1, 1)
    row_scale = 10.0 ** jax.random.uniform(key_rows, (1, SUBDOMAINS, NR), jnp.float32)
    base = jax.random.truncated_normal(key_base, -4.0, 4.0, (NCASE, SUBDOMAINS, NR), jnp.float32)
    ramp = 3.0 ** position
    return 0.04 * base * ramp[None, :, None] * row_scale


def shard_levels(rng, dims, cuts, low, largest):
    level, own = 1.0, jax.random.fold_in(rng, 6)
    for axis_at, blocks in cuts:
        draws = jnp.exp(jax.random.uniform(jax.random.fold_in(own, axis_at), (blocks,), jnp.float32, low / len(cuts), largest / len(cuts)))
        level = level * jnp.repeat(draws, dims[axis_at] // blocks).reshape([-1 if axis == axis_at else 1 for axis in range(len(dims))])
    return level


def gaussian(stream_key, dims, scale, most, shards=(), kind=jnp.bfloat16):
    values = jax.random.normal(stream_key, dims, jnp.float32) * scale
    if len(shards) > 0:
        values = shard_levels(stream_key, dims, shards, -0.22, 0.18) * values
    return jnp.clip(values, min=-most, max=most).astype(kind)


def setup_inputs(seed: int = 0) -> dict:
    key_of = jax.random.split(jax.random.key(seed), 11)
    return {
        "rr_inverse": draw_rr_inverse(jax.random.fold_in(key_of[10], 71), 0),
        "corner_modes": gaussian(key_of[1], (SUBDOMAINS, 2 * NC, NR), (NR // 4) ** -0.5, 0.5, ((0, 32),), jnp.float32),
        "coarse_inverse": draw_coarse_inverse(jax.random.fold_in(key_of[10], 71), 0),
        "inertia": jnp.clip(jnp.exp(math.log(2.0) - 1.3862944 * jax.random.uniform(key_of[3], (SUBDOMAINS, NR), jnp.float32) ** shard_levels(key_of[3], (SUBDOMAINS, NR), ((0, 32),), -0.2, 0.2)), 0.5, 2.0),
        "disp_now": gaussian(key_of[4], (NCASE, SUBDOMAINS, NR), 1.0, 4.0, ((1, 32),), jnp.float32),
        "vel_now": gaussian(key_of[5], (NCASE, SUBDOMAINS, NR), 1.0, 4.0, ((1, 32),), jnp.float32),
        "acc_now": gaussian(key_of[6], (NCASE, SUBDOMAINS, NR), 2.0, 8.0, ((1, 32),), jnp.float32),
        "load_next": draw_load_next(jax.random.fold_in(key_of[10], 71), 0),
        "basis_rows": gaussian(key_of[8], (NROWS, RANK), NROWS ** -0.5, 0.03125, ((0, 32),), jnp.float32),
        "piece_owner": jax.random.permutation(key_of[9], PIECES).astype(jnp.int32),
    }


highest = lax.Precision.HIGHEST
time_step = 0.5
newmark_beta = 0.25
newmark_gamma = 0.5

def green_apply(rr_inverse, corner_modes, coarse_inverse, field):

    def products(operands):
        return jnp.dot(operands[0], operands[1], precision=highest)
    local_part = lax.map(products, (rr_inverse, jnp.transpose(field, (1, 2, 0))))
    local_part = jnp.transpose(local_part, (2, 0, 1))
    corner_terms = jnp.einsum('kmb,ckb->ckm', corner_modes, field, precision=highest)
    assembled = corner_terms[:, :, NC:] + jnp.roll(corner_terms[:, :, :NC], -1, axis=1)
    coarse_rhs = assembled.reshape(NCASE, NCG)
    coarse_sol = lax.dot_general(coarse_rhs, coarse_inverse, (((1,), (1,)), ((), ())), precision=highest)
    coarse_sol = coarse_sol.reshape(NCASE, SUBDOMAINS, NC)
    coarse_values = jnp.concatenate([jnp.roll(coarse_sol, 1, axis=1), coarse_sol], axis=2)
    return local_part + jnp.einsum('kmb,ckm->ckb', corner_modes, coarse_values, precision=highest)

def interface_jump(field):
    return field[:, :, NR - NI:] - jnp.roll(field[:, :, :NI], -1, axis=1)

def spread(values):
    middle = jnp.zeros((NCASE, SUBDOMAINS, NR - 2 * NI), jnp.float32)
    return jnp.concatenate([-jnp.roll(values, 1, axis=1), middle, values], axis=2)

def reference(rr_inverse, corner_modes, coarse_inverse, inertia, disp_now, vel_now, acc_now, load_next, basis_rows, piece_owner):
    right_side = load_next + inertia[None] * (disp_now + time_step * vel_now + (0.5 - newmark_beta) * time_step * time_step * acc_now)
    green_rhs = green_apply(rr_inverse, corner_modes, coarse_inverse, right_side)
    residual = interface_jump(green_rhs)
    multipliers = jnp.zeros_like(residual)
    direction = residual
    norm_now = lax.optimization_barrier(jnp.sum(residual * residual, axis=(1, 2)))
    for iteration in range(ITERS):
        image = interface_jump(green_apply(rr_inverse, corner_modes, coarse_inverse, spread(direction)))
        curvature = lax.optimization_barrier(jnp.sum(direction * image, axis=(1, 2)))
        alpha = (norm_now / curvature)[:, None, None]
        multipliers = multipliers + alpha * direction
        residual = residual - alpha * image
        norm_next = lax.optimization_barrier(jnp.sum(residual * residual, axis=(1, 2)))
        direction = residual + (norm_next / norm_now)[:, None, None] * direction
        norm_now = norm_next
    disp_new = green_apply(rr_inverse, corner_modes, coarse_inverse, right_side - spread(multipliers))
    accel_new = (disp_new - disp_now) / (newmark_beta * time_step * time_step) - vel_now / (newmark_beta * time_step) - (0.5 / newmark_beta - 1.0) * acc_now
    vel_new = vel_now + time_step * ((1.0 - newmark_gamma) * acc_now + newmark_gamma * accel_new)
    inverse = jnp.zeros((PIECES,), jnp.int32).at[piece_owner].set(jnp.arange(PIECES, dtype=jnp.int32))
    piece_rows = NR // PIECES
    snapshots = disp_new.reshape(NCASE, SUBDOMAINS, PIECES, piece_rows)[:, :, inverse, :]
    snapshots = jnp.transpose(snapshots, (0, 2, 1, 3)).reshape(NCASE, NROWS)
    projection = lax.dot_general(basis_rows, snapshots, (((0,), (1,)), ((), ())), precision=highest)
    remainder = snapshots - lax.dot_general(projection, basis_rows, (((0,), (1,)), ((), ())), precision=highest)
    gram = lax.dot_general(remainder, remainder, (((1,), (1,)), ((), ())), precision=highest)
    lower = jnp.linalg.cholesky(gram)
    scale_rows = math.sqrt(NROWS)
    new_columns = jax.scipy.linalg.solve_triangular(lower, remainder, lower=True) * scale_rows
    r_factor = lower.T / scale_rows
    return (disp_new, vel_new, projection, r_factor, new_columns)
```

```python
import functools
import math

import jax
import jax.numpy as jnp
from jax import lax
from jax.experimental import pallas as pl
from jax.experimental.pallas import tpu as pltpu
from jax.sharding import PartitionSpec as P

NC = 32
NI = 128
LANES = 128

time_step = 0.5
newmark_beta = 0.25
newmark_gamma = 0.5

MESH = pl.DeviceIdType.MESH


def nn(a, b):
    return lax.dot_general(
        a, b, (((1,), (0,)), ((), ())), precision=lax.Precision.HIGHEST, preferred_element_type=jnp.float32
    )


def nt(a, b):
    return lax.dot_general(
        a, b, (((1,), (1,)), ((), ())), precision=lax.Precision.HIGHEST, preferred_element_type=jnp.float32
    )


def kernel(
    n,
    groups,
    inverse,
    rr_hbm,
    modes_hbm,
    coarse_hbm,
    basis_hbm,
    inertia,
    disp_now,
    vel_now,
    acc_now,
    load_next,
    disp_out,
    vel_out,
    proj_out,
    r_out,
    cols_out,
    rr,
    modes,
    coarse,
    basis,
    modes_next,
    rr_next,
    corner,
    inter,
    gathered,
    edge,
    edge_out,
    norms,
    pieces,
    outgoing,
    incoming,
    proj_parts,
    gram_parts,
    green,
    local_sem,
    const_send,
    const_recv,
    wide_send,
    wide_recv,
    edge_send,
    edge_recv,
):
    sub_count, unknowns = rr.shape[0], rr.shape[1]
    rows = sub_count * NC
    me = lax.axis_index("sub") * groups + lax.axis_index("grp")
    following = lax.rem(me + 1, n)
    earlier = lax.rem(me + n - 1, n)

    def device(rank):
        return (rank // groups, lax.rem(rank, groups))

    def others(body):
        def step(i, carry):
            body(lax.rem(me + i, n))
            return carry

        lax.fori_loop(1, n, step, 0)

    def remote(src, dst, send, recv, rank):
        return pltpu.make_async_remote_copy(
            src_ref=src, dst_ref=dst, send_sem=send, recv_sem=recv, device_id=device(rank), device_id_type=MESH
        )

    barrier = pltpu.get_barrier_semaphore()
    others(lambda rank: pl.semaphore_signal(barrier, inc=1, device_id=device(rank), device_id_type=MESH))

    load_rr = pltpu.make_async_copy(rr_hbm, rr, local_sem.at[0])
    load_modes = pltpu.make_async_copy(modes_hbm, modes, local_sem.at[1])
    load_coarse = pltpu.make_async_copy(coarse_hbm, coarse.at[pl.ds(0, rows)], local_sem.at[2])
    load_basis = pltpu.make_async_copy(basis_hbm, basis, local_sem.at[3])
    load_modes.start()
    load_rr.start()
    load_coarse.start()
    load_basis.start()

    lane = lax.broadcasted_iota(jnp.int32, (8, LANES), 1)
    sublane = lax.broadcasted_iota(jnp.int32, (8, LANES), 0)

    def right_side(k):
        return load_next[:, k, :] + inertia[k : k + 1, :] * (
            disp_now[:, k, :]
            + time_step * vel_now[:, k, :]
            + (0.5 - newmark_beta) * time_step * time_step * acc_now[:, k, :]
        )

    sides = [right_side(k) for k in range(sub_count)]

    corner[...] = jnp.zeros_like(corner)
    load_modes.wait()
    corner[0:NC, 0:unknowns] = modes[0, NC:, :]
    corner[0:NC, unknowns:] = modes[1, :NC, :]
    corner[NC : 2 * NC, unknowns:] = modes[1, NC:, :]
    corner[3 * NC :, 0:unknowns] = modes[0, :NC, :]

    odd = lax.rem(me, 2) == 1

    def placed(tile):
        return jnp.where(odd, pltpu.roll(tile, 64, 1), tile)

    def broadcast(buffer, at, sem):
        def send(rank):
            remote(buffer.at[at, me], buffer.at[at, me], wide_send.at[sem], wide_recv.at[sem], rank).start()

        others(send)

    def all_but_one(buffer, at, sem):
        return pltpu.make_async_copy(buffer.at[at, pl.ds(0, n - 1)], buffer.at[at, pl.ds(0, n - 1)], sem)

    gathered[0, me] = placed(nt(jnp.concatenate(sides, axis=1), corner[...]))

    pl.semaphore_wait(barrier, n - 1)
    broadcast(gathered, 0, 0)

    constants = [
        remote(coarse_hbm.at[pl.ds(0, NC)], coarse.at[pl.ds(rows, NC)], const_send.at[0], const_recv.at[0], earlier),
        remote(
            coarse_hbm.at[pl.ds(rows - NC, NC)],
            coarse.at[pl.ds(rows + NC, NC)],
            const_send.at[1],
            const_recv.at[1],
            following,
        ),
        remote(modes_hbm.at[0, :, pl.ds(0, NI)], modes_next, const_send.at[2], const_recv.at[2], earlier),
        remote(
            rr_hbm.at[0, pl.ds(0, NI), pl.ds(0, NI)],
            rr_next.at[pl.ds(0, NI)],
            const_send.at[3],
            const_recv.at[3],
            earlier,
        ),
        remote(
            rr_hbm.at[0, pl.ds(unknowns - NI, NI), pl.ds(0, NI)],
            rr_next.at[pl.ds(NI, NI)],
            const_send.at[4],
            const_recv.at[4],
            earlier,
        ),
    ]
    for copy in constants:
        copy.start()

    load_rr.wait()
    local = [nn(sides[k], rr[k]) for k in range(sub_count)]
    edge_out[0] = local[0][:, :NI]
    edges = [remote(edge_out.at[0], edge.at[0], edge_send.at[0], edge_recv.at[0], earlier)]
    edges[0].start()

    load_coarse.wait()
    for copy in constants:
        copy.wait_recv()
    inter[...] = jnp.zeros_like(inter)
    inter[0:NC, 0:NI] = modes[0, NC:, unknowns - NI :] - modes[1, :NC, :NI]
    inter[0:NC, NI:] = modes[1, :NC, unknowns - NI :]
    inter[NC : 2 * NC, 0:NI] = -modes[1, NC:, :NI]
    inter[NC : 2 * NC, NI:] = modes[1, NC:, unknowns - NI :] - modes_next[:NC, :]
    inter[2 * NC : 3 * NC, NI:] = -modes_next[NC:, :]
    inter[3 * NC :, 0:NI] = modes[0, :NC, unknowns - NI :]

    def coarse_solve(at):
        all_but_one(gathered, at, wide_recv.at[at]).wait()
        assembled = []
        for j in range(n // 2):
            low = jnp.where(lane < 96, gathered[at, 2 * j], gathered[at, (2 * j + 2) % n])
            high = jnp.where(lane >= 32, gathered[at, 2 * j + 1], gathered[at, (2 * j - 1) % n])
            assembled.append(low + high)
        return nt(jnp.concatenate(assembled, axis=1), coarse[...])

    def jumps(fields, next_first):
        firsts = [field[:, :NI] for field in fields[1:]] + [next_first]
        return jnp.concatenate(
            [field[:, unknowns - NI :] - first for field, first in zip(fields, firsts)], axis=1
        )

    per_piece = unknowns // n
    width = sub_count * per_piece

    def piece_part(fields, which, p):
        block = p * per_piece // LANES
        inside = p * per_piece % LANES
        part = jnp.zeros((8, LANES), jnp.float32)
        for k in range(sub_count):
            target = which * width + k * per_piece
            rolled = pltpu.roll(
                fields[k][:, block * LANES : (block + 1) * LANES], (target - inside) % LANES, 1
            )
            part = jnp.where((lane >= target) & (lane < target + per_piece), rolled, part)
        return part

    solved = coarse_solve(0)
    edges[0].wait_recv()
    first_fields = [
        local[k] + nn(solved, corner[:, k * unknowns : (k + 1) * unknowns]) for k in range(sub_count)
    ]
    vector0 = jumps(local, edge[0]) + nn(solved, inter[...])

    def start_image(vector, at):
        gathered[at, me] = placed(nt(vector, inter[...]))
        broadcast(gathered, at, at)
        slot = 2 * at - 1
        edge_out[slot] = vector[:, NI:]
        edge_out[slot + 1] = vector[:, :NI]
        for offset, rank in ((0, following), (1, earlier)):
            copy = remote(
                edge_out.at[slot + offset],
                edge.at[slot + offset],
                edge_send.at[slot + offset],
                edge_recv.at[slot + offset],
                rank,
            )
            copy.start()
            edges.append(copy)

    def end_image(vector, at):
        slot = 2 * at - 1
        head, tail = vector[:, :NI], vector[:, NI:]
        second = nn(-head, rr[1, :NI, :]) + nn(tail, rr[1, unknowns - NI :, :])
        edges[slot].wait_recv()
        edges[slot + 1].wait_recv()
        first = nn(-edge[slot], rr[0, :NI, :]) + nn(head, rr[0, unknowns - NI :, :])
        beyond = nn(-tail, rr_next[:NI, :]) + nn(edge[slot + 1], rr_next[NI:, :])
        inner = [first, second]
        values = coarse_solve(at)
        fields = [
            inner[k] + nn(values, corner[:, k * unknowns : (k + 1) * unknowns]) for k in range(sub_count)
        ]
        return fields, jumps(inner, beyond) + nn(values, inter[...])

    def column(values):
        return jnp.sum(values, axis=1, keepdims=True)

    start_image(vector0, 1)
    for k in range(sub_count):
        green[k] = first_fields[k]
    for p in range(n):
        pieces[p] = piece_part(first_fields, 0, p)
    fields0, vector1 = end_image(vector0, 1)

    start_image(vector1, 2)
    norm_row = jnp.where(lane == sublane, column(vector0 * vector0), 0.0) + jnp.where(
        lane == sublane + 8, column(vector0 * vector1), 0.0
    )
    norms[0, me] = jnp.sum(norm_row, axis=0, keepdims=True)
    broadcast(norms, 0, 3)
    for p in range(n):
        pieces[p] = pieces[p] + piece_part(fields0, 1, p)
    fields1, vector2 = end_image(vector1, 2)

    all_but_one(norms, 0, wide_recv.at[3]).wait()
    totals = jnp.broadcast_to(jnp.sum(norms[0], axis=0), (8, LANES))
    norm0 = column(jnp.where(lane == sublane, totals, 0.0))
    curve0 = column(jnp.where(lane == sublane + 8, totals, 0.0))
    alpha0 = norm0 / curve0
    residual = vector0 - alpha0 * vector1
    residual_image = vector1 - alpha0 * vector2
    extra = (
        jnp.where(lane == 3 * width, column(residual * residual), 0.0)
        + jnp.where(lane == 3 * width + 1, column(residual * residual_image), 0.0)
        + jnp.where(lane == 3 * width + 2, column(residual * vector1), 0.0)
    )
    for p in range(n):
        pieces[p] = pieces[p] + piece_part(fields1, 2, p) + extra
    for t in range(n):
        outgoing[t] = pieces[inverse[t]]

    def send_piece(rank):
        remote(outgoing.at[rank], incoming.at[0, me], wide_send.at[4], wide_recv.at[4], rank).start()

    others(send_piece)
    incoming[0, me] = outgoing[me]
    load_basis.wait()
    all_but_one(incoming, 0, wide_recv.at[4]).wait()

    sums = jnp.sum(incoming[0], axis=0)
    norm1 = column(jnp.where(lane == 3 * width, sums, 0.0))
    curve_rr = column(jnp.where(lane == 3 * width + 1, sums, 0.0))
    curve_rp = column(jnp.where(lane == 3 * width + 2, sums, 0.0))
    beta = norm1 / norm0
    curve1 = curve_rr + 2.0 * beta * curve_rp + beta * beta * curve0
    alpha1 = norm1 / curve1
    scale0 = alpha0 + alpha1 * (1.0 + beta)
    scale1 = -alpha1 * alpha0

    factor = jnp.where(lane < width, 1.0, jnp.where(lane < 2 * width, -scale0, -scale1))
    factor = jnp.where(lane < 3 * width, factor, 0.0)
    per_tile = LANES // width
    snapshot_tiles = []
    for j in range(n // per_tile):
        tile = jnp.zeros((8, LANES), jnp.float32)
        for i in range(per_tile):
            scaled = incoming[0, j * per_tile + i] * factor
            total = scaled
            for which in (1, 2):
                total = total + pltpu.roll(scaled, LANES - which * width, 1)
            if i:
                total = pltpu.roll(total, i * width, 1)
            tile = jnp.where((lane >= i * width) & (lane < (i + 1) * width), total, tile)
        snapshot_tiles.append(tile)
    snapshots = jnp.concatenate(snapshot_tiles, axis=1)
    proj_parts[0, me] = nn(snapshots, basis[...])
    broadcast(proj_parts, 0, 5)

    for k in range(sub_count):
        carried = green[k] - scale0 * fields0[k] - scale1 * fields1[k]
        now, vel, acc = disp_now[:, k, :], vel_now[:, k, :], acc_now[:, k, :]
        accel_new = (
            (carried - now) / (newmark_beta * time_step * time_step)
            - vel / (newmark_beta * time_step)
            - (0.5 / newmark_beta - 1.0) * acc
        )
        disp_out[:, k, :] = carried
        vel_out[:, k, :] = vel + time_step * ((1.0 - newmark_gamma) * acc + newmark_gamma * accel_new)

    all_but_one(proj_parts, 0, wide_recv.at[5]).wait()
    projection = jnp.sum(proj_parts[0], axis=0)
    proj_out[...] = projection
    remainder = snapshots - nt(projection, basis[...])
    repeated = jnp.concatenate([remainder] * (LANES // 8), axis=0)
    gram_wide = nt(remainder, repeated)
    gram_parts[0, me] = jnp.sum(
        jnp.where(lane // 8 == sublane, gram_wide, 0.0), axis=0, keepdims=True
    )
    broadcast(gram_parts, 0, 6)
    all_but_one(gram_parts, 0, wide_recv.at[6]).wait()
    gram_row = jnp.broadcast_to(jnp.sum(gram_parts[0], axis=0), (8, LANES))
    work = gram_row
    for i in range(1, 8):
        work = jnp.where(sublane == i, pltpu.roll(gram_row, LANES - 8 * i, 1), work)
    for j in range(8):
        inverse_root = lax.rsqrt(work[j : j + 1, j : j + 1])
        pivot = work[j : j + 1, :] * inverse_root
        below = work[:, j : j + 1] * inverse_root
        pivot_rows = remainder[j : j + 1, :] * inverse_root
        work = jnp.where(sublane == j, pivot, jnp.where(sublane > j, work - below * pivot, work))
        row_at = lax.broadcasted_iota(jnp.int32, remainder.shape, 0)
        remainder = jnp.where(
            row_at == j, pivot_rows, jnp.where(row_at > j, remainder - below * pivot_rows, remainder)
        )
    scale_rows = math.sqrt(snapshots.shape[1] * n)
    r_out[...] = jnp.where(lane >= sublane, work, 0.0)[:, :8] * (1.0 / scale_rows)
    cols_out[...] = remainder * scale_rows

    for copy in constants + edges:
        copy.wait_send()
    for at in range(3):
        all_but_one(gathered, at, wide_send.at[at]).wait()
    all_but_one(norms, 0, wide_send.at[3]).wait()
    all_but_one(incoming, 0, wide_send.at[4]).wait()
    all_but_one(proj_parts, 0, wide_send.at[5]).wait()
    all_but_one(gram_parts, 0, wide_send.at[6]).wait()


def solution(mesh):
    groups = mesh.shape["grp"]
    n = mesh.shape["sub"] * groups

    def shards(
        rr_inverse,
        corner_modes,
        coarse_inverse,
        inertia,
        disp_now,
        vel_now,
        acc_now,
        load_next,
        basis_rows,
        piece_owner,
    ):
        case_count, sub_count, unknowns = disp_now.shape
        rank = basis_rows.shape[1]
        local_rows = basis_rows.shape[0]
        counting = jnp.arange(n, dtype=jnp.int32)
        inverse = jnp.sum(
            jnp.where(piece_owner[None, :] == counting[:, None], counting[None, :], 0), axis=1, dtype=jnp.int32
        )
        width = (sub_count + 2) * NC
        f32 = jnp.float32
        vmem = pl.BlockSpec(memory_space=pltpu.VMEM)
        anywhere = pl.BlockSpec(memory_space=pl.ANY)
        disp, vel, proj, r_factor, columns = pl.pallas_call(
            functools.partial(kernel, n, groups),
            out_shape=(
                jax.ShapeDtypeStruct(disp_now.shape, f32),
                jax.ShapeDtypeStruct(disp_now.shape, f32),
                jax.ShapeDtypeStruct((case_count, rank), f32),
                jax.ShapeDtypeStruct((case_count, case_count), f32),
                jax.ShapeDtypeStruct((case_count, local_rows), f32),
            ),
            in_specs=[pl.BlockSpec(memory_space=pltpu.SMEM)] + [anywhere] * 4 + [vmem] * 5,
            out_specs=(vmem,) * 5,
            scratch_shapes=[
                pltpu.VMEM(rr_inverse.shape, f32),
                pltpu.VMEM(corner_modes.shape, f32),
                pltpu.VMEM((width, coarse_inverse.shape[1]), f32),
                pltpu.VMEM(basis_rows.shape, f32),
                pltpu.VMEM((2 * NC, NI), f32),
                pltpu.VMEM((2 * NI, NI), f32),
                pltpu.VMEM((width, sub_count * unknowns), f32),
                pltpu.VMEM((width, sub_count * NI), f32),
                pltpu.VMEM((3, n, case_count, width), f32),
                pltpu.VMEM((5, case_count, NI), f32),
                pltpu.VMEM((5, case_count, NI), f32),
                pltpu.VMEM((1, n, 1, LANES), f32),
                pltpu.VMEM((n, case_count, LANES), f32),
                pltpu.VMEM((n, case_count, LANES), f32),
                pltpu.VMEM((1, n, case_count, LANES), f32),
                pltpu.VMEM((1, n, case_count, rank), f32),
                pltpu.VMEM((1, n, 1, LANES), f32),
                pltpu.VMEM((sub_count, case_count, unknowns), f32),
                pltpu.SemaphoreType.DMA((4,)),
                pltpu.SemaphoreType.DMA((5,)),
                pltpu.SemaphoreType.DMA((5,)),
                pltpu.SemaphoreType.DMA((7,)),
                pltpu.SemaphoreType.DMA((7,)),
                pltpu.SemaphoreType.DMA((5,)),
                pltpu.SemaphoreType.DMA((5,)),
            ],
            compiler_params=pltpu.CompilerParams(collective_id=0, has_side_effects=True),
        )(
            inverse,
            rr_inverse,
            corner_modes,
            coarse_inverse,
            basis_rows,
            inertia,
            disp_now,
            vel_now,
            acc_now,
            load_next,
        )
        return disp, vel, proj.T, r_factor, columns

    return jax.shard_map(
        shards,
        mesh=mesh,
        in_specs=(
            P(("sub", "grp"), None, None),
            P(("sub", "grp"), None, None),
            P(("sub", "grp"), None),
            P(("sub", "grp"), None),
            P(None, ("sub", "grp"), None),
            P(None, ("sub", "grp"), None),
            P(None, ("sub", "grp"), None),
            P(None, ("sub", "grp"), None),
            P(("sub", "grp"), None),
            P(),
        ),
        out_specs=(
            P(None, ("sub", "grp"), None),
            P(None, ("sub", "grp"), None),
            P(),
            P(),
            P(None, ("sub", "grp")),
        ),
        check_vma=False,
    )
```

```python
import functools
import math

import jax
import jax.numpy as jnp
from jax import lax
from jax.experimental import pallas as pl
from jax.experimental.pallas import tpu as pltpu
from jax.sharding import PartitionSpec as P

NC = 32
NI = 128
LANES = 128

time_step = 0.5
newmark_beta = 0.25
newmark_gamma = 0.5

MESH = pl.DeviceIdType.MESH


def nn(a, b):
    return lax.dot_general(
        a, b, (((1,), (0,)), ((), ())), precision=lax.Precision.HIGHEST, preferred_element_type=jnp.float32
    )


def nt(a, b):
    return lax.dot_general(
        a, b, (((1,), (1,)), ((), ())), precision=lax.Precision.HIGHEST, preferred_element_type=jnp.float32
    )


def split(x):
    first = x.astype(jnp.bfloat16)
    rest = x - first.astype(jnp.float32)
    second = rest.astype(jnp.bfloat16)
    return first, second, (rest - second.astype(jnp.float32)).astype(jnp.bfloat16)


def keep_split(parts, matrix):
    for at, part in enumerate(split(matrix)):
        parts[at] = part


def split_dot(x, parts, contracted):
    first, second, third = split(x)
    stacked = jnp.concatenate([first, second, third, jnp.zeros_like(first)], axis=0)
    rows = x.shape[0]

    def product(a, b):
        return lax.dot_general(a, b, (((1,), (contracted,)), ((), ())), preferred_element_type=jnp.float32)

    large = product(stacked, parts[0])
    middle = product(stacked[: 2 * rows], parts[1])
    small = product(stacked[: 2 * rows], parts[2])
    correction = large[2 * rows : 3 * rows] + middle[rows : 2 * rows] + small[:rows]
    return large[:rows] + (large[rows : 2 * rows] + middle[:rows] + correction)


def hand_over(*refs):
    half = len(refs) // 2
    for source, target in zip(refs[:half], refs[half:]):
        target[...] = source[...]


def kernel(
    n,
    groups,
    inner,
    owner_hbm,
    rr_hbm,
    modes_hbm,
    coarse_hbm,
    basis_hbm,
    inertia_hbm,
    disp_hbm,
    vel_hbm,
    acc_hbm,
    load_hbm,
    disp_out,
    vel_out,
    proj_out,
    r_out,
    cols_out,
    owner,
    inverse,
    inertia,
    disp_now,
    vel_now,
    acc_now,
    load_next,
    coarse_parts,
    inter_parts,
    basis_parts,
    rr,
    modes,
    coarse,
    basis,
    modes_next,
    rr_next,
    corner,
    inter,
    gathered,
    edge,
    edge_out,
    norms,
    pieces,
    outgoing,
    incoming,
    proj_parts,
    proj_sums,
    gram_parts,
    green,
    local_sem,
    const_send,
    const_recv,
    wide_send,
    wide_recv,
    edge_send,
    edge_recv,
):
    sub_count, unknowns = rr.shape[0], rr.shape[1]
    rows = sub_count * NC
    me = lax.axis_index("sub") * groups + lax.axis_index("grp")
    following = lax.rem(me + 1, n)
    earlier = lax.rem(me + n - 1, n)

    def device(rank):
        return (rank // groups, lax.rem(rank, groups))

    def others(body):
        def step(i, carry):
            body(lax.rem(me + i, n))
            return carry

        lax.fori_loop(1, n, step, 0)

    def remote(src, dst, send, recv, rank):
        return pltpu.make_async_remote_copy(
            src_ref=src, dst_ref=dst, send_sem=send, recv_sem=recv, device_id=device(rank), device_id_type=MESH
        )

    barrier = pltpu.get_barrier_semaphore()
    others(lambda rank: pl.semaphore_signal(barrier, inc=1, device_id=device(rank), device_id_type=MESH))

    load_rr = pltpu.make_async_copy(rr_hbm, rr, local_sem.at[0])
    load_modes = pltpu.make_async_copy(modes_hbm, modes, local_sem.at[1])
    load_coarse = pltpu.make_async_copy(coarse_hbm, coarse.at[pl.ds(0, rows)], local_sem.at[2])
    load_basis = pltpu.make_async_copy(basis_hbm, basis, local_sem.at[3])
    fields_in = [
        pltpu.make_async_copy(source, target, local_sem.at[4 + at])
        for at, (source, target) in enumerate(
            (
                (inertia_hbm, inertia),
                (disp_hbm, disp_now),
                (vel_hbm, vel_now),
                (acc_hbm, acc_now),
                (load_hbm, load_next),
            )
        )
    ]
    load_owner = pltpu.make_async_copy(owner_hbm, owner, local_sem.at[9])
    load_modes.start()
    for copy in fields_in:
        copy.start()
    load_owner.start()
    load_rr.start()
    load_coarse.start()
    load_basis.start()

    lane = lax.broadcasted_iota(jnp.int32, (8, LANES), 1)
    sublane = lax.broadcasted_iota(jnp.int32, (8, LANES), 0)

    def right_side(k):
        return load_next[:, k, :] + inertia[k : k + 1, :] * (
            disp_now[:, k, :]
            + time_step * vel_now[:, k, :]
            + (0.5 - newmark_beta) * time_step * time_step * acc_now[:, k, :]
        )

    for copy in fields_in:
        copy.wait()
    sides = [right_side(k) for k in range(sub_count)]

    corner[...] = jnp.zeros_like(corner)
    load_modes.wait()
    corner[0:NC, 0:unknowns] = modes[0, NC:, :]
    corner[0:NC, unknowns:] = modes[1, :NC, :]
    corner[NC : 2 * NC, unknowns:] = modes[1, NC:, :]
    corner[3 * NC :, 0:unknowns] = modes[0, :NC, :]

    odd = lax.rem(me, 2) == 1

    def placed(tile):
        return jnp.where(odd, pltpu.roll(tile, 64, 1), tile)

    def broadcast(buffer, at, sem):
        def send(rank):
            remote(buffer.at[at, me], buffer.at[at, me], wide_send.at[sem], wide_recv.at[sem], rank).start()

        others(send)

    def all_but_one(buffer, at, sem):
        return pltpu.make_async_copy(buffer.at[at, pl.ds(0, n - 1)], buffer.at[at, pl.ds(0, n - 1)], sem)

    gathered[0, me] = placed(nt(jnp.concatenate(sides, axis=1), corner[...]))

    pl.semaphore_wait(barrier, n - 1)
    broadcast(gathered, 0, 0)

    constants = [
        remote(coarse_hbm.at[pl.ds(0, NC)], coarse.at[pl.ds(rows, NC)], const_send.at[0], const_recv.at[0], earlier),
        remote(
            coarse_hbm.at[pl.ds(rows - NC, NC)],
            coarse.at[pl.ds(rows + NC, NC)],
            const_send.at[1],
            const_recv.at[1],
            following,
        ),
        remote(modes_hbm.at[0, :, pl.ds(0, NI)], modes_next, const_send.at[2], const_recv.at[2], earlier),
        remote(
            rr_hbm.at[0, pl.ds(0, NI), pl.ds(0, NI)],
            rr_next.at[pl.ds(0, NI)],
            const_send.at[3],
            const_recv.at[3],
            earlier,
        ),
        remote(
            rr_hbm.at[0, pl.ds(unknowns - NI, NI), pl.ds(0, NI)],
            rr_next.at[pl.ds(NI, NI)],
            const_send.at[4],
            const_recv.at[4],
            earlier,
        ),
    ]
    for copy in constants:
        copy.start()

    load_rr.wait()
    local = [nn(sides[k], rr[k]) for k in range(sub_count)]
    edge_out[0] = local[0][:, :NI]
    edges = [remote(edge_out.at[0], edge.at[0], edge_send.at[0], edge_recv.at[0], earlier)]
    edges[0].start()

    load_coarse.wait()
    for copy in constants:
        copy.wait_recv()
    inter[...] = jnp.zeros_like(inter)
    inter[0:NC, 0:NI] = modes[0, NC:, unknowns - NI :] - modes[1, :NC, :NI]
    inter[0:NC, NI:] = modes[1, :NC, unknowns - NI :]
    inter[NC : 2 * NC, 0:NI] = -modes[1, NC:, :NI]
    inter[NC : 2 * NC, NI:] = modes[1, NC:, unknowns - NI :] - modes_next[:NC, :]
    inter[2 * NC : 3 * NC, NI:] = -modes_next[NC:, :]
    inter[3 * NC :, 0:NI] = modes[0, :NC, unknowns - NI :]

    keep_split(inter_parts, inter[...])
    keep_split(coarse_parts, coarse[...])
    load_owner.wait()

    def find(t, carry):
        at = jnp.int32(0)
        for p in range(n):
            at = jnp.where(owner[p] == t, p, at)
        inverse[t] = at
        return carry

    lax.fori_loop(0, n, find, 0)

    def coarse_solve(at):
        all_but_one(gathered, at, wide_recv.at[at]).wait()
        assembled = []
        for j in range(n // 2):
            low = jnp.where(lane < 96, gathered[at, 2 * j], gathered[at, (2 * j + 2) % n])
            high = jnp.where(lane >= 32, gathered[at, 2 * j + 1], gathered[at, (2 * j - 1) % n])
            assembled.append(low + high)
        return split_dot(jnp.concatenate(assembled, axis=1), coarse_parts, 1)

    def jumps(fields, next_first):
        firsts = [field[:, :NI] for field in fields[1:]] + [next_first]
        return jnp.concatenate(
            [field[:, unknowns - NI :] - first for field, first in zip(fields, firsts)], axis=1
        )

    per_piece = unknowns // n
    width = sub_count * per_piece

    def piece_part(fields, which, p):
        block = p * per_piece // LANES
        inside = p * per_piece % LANES
        part = jnp.zeros((8, LANES), jnp.float32)
        for k in range(sub_count):
            target = which * width + k * per_piece
            rolled = pltpu.roll(
                fields[k][:, block * LANES : (block + 1) * LANES], (target - inside) % LANES, 1
            )
            part = jnp.where((lane >= target) & (lane < target + per_piece), rolled, part)
        return part

    solved = coarse_solve(0)
    edges[0].wait_recv()
    vector0 = jumps(local, edge[0]) + split_dot(solved, inter_parts, 0)

    def start_image(vector, at):
        gathered[at, me] = placed(split_dot(vector, inter_parts, 1))
        broadcast(gathered, at, at)
        slot = 2 * at - 1
        edge_out[slot] = vector[:, NI:]
        edge_out[slot + 1] = vector[:, :NI]
        for offset, rank in ((0, following), (1, earlier)):
            copy = remote(
                edge_out.at[slot + offset],
                edge.at[slot + offset],
                edge_send.at[slot + offset],
                edge_recv.at[slot + offset],
                rank,
            )
            copy.start()
            edges.append(copy)

    def end_image(vector, at):
        slot = 2 * at - 1
        head, tail = vector[:, :NI], vector[:, NI:]
        second = nn(-head, rr[1, :NI, :]) + nn(tail, rr[1, unknowns - NI :, :])
        edges[slot].wait_recv()
        edges[slot + 1].wait_recv()
        first = nn(-edge[slot], rr[0, :NI, :]) + nn(head, rr[0, unknowns - NI :, :])
        beyond = nn(-tail, rr_next[:NI, :]) + nn(edge[slot + 1], rr_next[NI:, :])
        inside = [first, second]
        values = coarse_solve(at)
        return inside, values, jumps(inside, beyond) + split_dot(values, inter_parts, 0)

    def with_corners(inside, values):
        return [
            inside[k] + nn(values, corner[:, k * unknowns : (k + 1) * unknowns]) for k in range(sub_count)
        ]

    def column(values):
        return jnp.sum(values, axis=1, keepdims=True)

    start_image(vector0, 1)
    first_fields = with_corners(local, solved)
    for k in range(sub_count):
        green[k] = first_fields[k]
    for p in range(n):
        pieces[p] = piece_part(first_fields, 0, p)
    inside0, values0, vector1 = end_image(vector0, 1)

    start_image(vector1, 2)
    norm_row = jnp.where(lane == sublane, column(vector0 * vector0), 0.0) + jnp.where(
        lane == sublane + 8, column(vector0 * vector1), 0.0
    )
    norms[0, me] = jnp.sum(norm_row, axis=0, keepdims=True)
    broadcast(norms, 0, 3)
    fields0 = with_corners(inside0, values0)
    for p in range(n):
        pieces[p] = pieces[p] + piece_part(fields0, 1, p)
    load_basis.wait()
    keep_split(basis_parts, basis[...])
    inside1, values1, vector2 = end_image(vector1, 2)
    fields1 = with_corners(inside1, values1)

    all_but_one(norms, 0, wide_recv.at[3]).wait()
    totals = jnp.broadcast_to(jnp.sum(norms[0], axis=0), (8, LANES))
    norm0 = column(jnp.where(lane == sublane, totals, 0.0))
    curve0 = column(jnp.where(lane == sublane + 8, totals, 0.0))
    alpha0 = norm0 / curve0
    residual = vector0 - alpha0 * vector1
    residual_image = vector1 - alpha0 * vector2
    extra = (
        jnp.where(lane == 3 * width, column(residual * residual), 0.0)
        + jnp.where(lane == 3 * width + 1, column(residual * residual_image), 0.0)
        + jnp.where(lane == 3 * width + 2, column(residual * vector1), 0.0)
    )
    for p in range(n):
        pieces[p] = pieces[p] + piece_part(fields1, 2, p) + extra
    for t in range(n):
        outgoing[t] = pieces[inverse[t]]

    def send_piece(rank):
        remote(outgoing.at[rank], incoming.at[0, me], wide_send.at[4], wide_recv.at[4], rank).start()

    others(send_piece)
    incoming[0, me] = outgoing[me]
    all_but_one(incoming, 0, wide_recv.at[4]).wait()

    sums = jnp.sum(incoming[0], axis=0)
    norm1 = column(jnp.where(lane == 3 * width, sums, 0.0))
    curve_rr = column(jnp.where(lane == 3 * width + 1, sums, 0.0))
    curve_rp = column(jnp.where(lane == 3 * width + 2, sums, 0.0))
    beta = norm1 / norm0
    curve1 = curve_rr + 2.0 * beta * curve_rp + beta * beta * curve0
    alpha1 = norm1 / curve1
    scale0 = alpha0 + alpha1 * (1.0 + beta)
    scale1 = -alpha1 * alpha0

    factor = jnp.where(lane < width, 1.0, jnp.where(lane < 2 * width, -scale0, -scale1))
    factor = jnp.where(lane < 3 * width, factor, 0.0)
    per_tile = LANES // width
    snapshot_tiles = []
    for j in range(n // per_tile):
        tile = jnp.zeros((8, LANES), jnp.float32)
        for i in range(per_tile):
            scaled = incoming[0, j * per_tile + i] * factor
            total = scaled
            for which in (1, 2):
                total = total + pltpu.roll(scaled, LANES - which * width, 1)
            if i:
                total = pltpu.roll(total, i * width, 1)
            tile = jnp.where((lane >= i * width) & (lane < (i + 1) * width), total, tile)
        snapshot_tiles.append(tile)
    snapshots = jnp.concatenate(snapshot_tiles, axis=1)
    plane, outer = me // inner, n // inner
    seat = lax.rem(me, inner)
    proj_parts[seat] = split_dot(snapshots, basis_parts, 0)
    for i in range(1, inner):
        rank = plane * inner + lax.rem(seat + i, inner)
        remote(proj_parts.at[seat], proj_parts.at[seat], wide_send.at[5], wide_recv.at[5], rank).start()

    for k in range(sub_count):
        carried = green[k] - scale0 * fields0[k] - scale1 * fields1[k]
        now, vel, acc = disp_now[:, k, :], vel_now[:, k, :], acc_now[:, k, :]
        accel_new = (
            (carried - now) / (newmark_beta * time_step * time_step)
            - vel / (newmark_beta * time_step)
            - (0.5 / newmark_beta - 1.0) * acc
        )
        disp_out[:, k, :] = carried
        vel_out[:, k, :] = vel + time_step * ((1.0 - newmark_gamma) * acc + newmark_gamma * accel_new)

    pltpu.make_async_copy(
        proj_parts.at[pl.ds(0, inner - 1)], proj_parts.at[pl.ds(0, inner - 1)], wide_recv.at[5]
    ).wait()
    proj_sums[plane] = jnp.sum(proj_parts[...], axis=0)
    for i in range(1, outer):
        rank = lax.rem(plane + i, outer) * inner + seat
        remote(proj_sums.at[plane], proj_sums.at[plane], wide_send.at[7], wide_recv.at[7], rank).start()
    pltpu.make_async_copy(
        proj_sums.at[pl.ds(0, outer - 1)], proj_sums.at[pl.ds(0, outer - 1)], wide_recv.at[7]
    ).wait()
    projection = jnp.sum(proj_sums[...], axis=0)
    proj_out[...] = projection
    remainder = snapshots - split_dot(projection, basis_parts, 1)
    repeated = jnp.concatenate([remainder] * (LANES // 8), axis=0)
    gram_wide = nt(remainder, repeated)
    gram_parts[0, me] = jnp.sum(
        jnp.where(lane // 8 == sublane, gram_wide, 0.0), axis=0, keepdims=True
    )
    broadcast(gram_parts, 0, 6)
    all_but_one(gram_parts, 0, wide_recv.at[6]).wait()
    gram_row = jnp.broadcast_to(jnp.sum(gram_parts[0], axis=0), (8, LANES))
    work = gram_row
    for i in range(1, 8):
        work = jnp.where(sublane == i, pltpu.roll(gram_row, LANES - 8 * i, 1), work)
    for j in range(8):
        inverse_root = lax.rsqrt(work[j : j + 1, j : j + 1])
        pivot = work[j : j + 1, :] * inverse_root
        below = work[:, j : j + 1] * inverse_root
        pivot_rows = remainder[j : j + 1, :] * inverse_root
        work = jnp.where(sublane == j, pivot, jnp.where(sublane > j, work - below * pivot, work))
        row_at = lax.broadcasted_iota(jnp.int32, remainder.shape, 0)
        remainder = jnp.where(
            row_at == j, pivot_rows, jnp.where(row_at > j, remainder - below * pivot_rows, remainder)
        )
    scale_rows = math.sqrt(snapshots.shape[1] * n)
    r_out[...] = jnp.where(lane >= sublane, work, 0.0)[:, :8] * (1.0 / scale_rows)
    cols_out[...] = remainder * scale_rows

    for copy in constants + edges:
        copy.wait_send()
    for at in range(3):
        all_but_one(gathered, at, wide_send.at[at]).wait()
    all_but_one(norms, 0, wide_send.at[3]).wait()
    all_but_one(incoming, 0, wide_send.at[4]).wait()
    pltpu.make_async_copy(
        proj_parts.at[pl.ds(0, inner - 1)], proj_parts.at[pl.ds(0, inner - 1)], wide_send.at[5]
    ).wait()
    pltpu.make_async_copy(
        proj_sums.at[pl.ds(0, outer - 1)], proj_sums.at[pl.ds(0, outer - 1)], wide_send.at[7]
    ).wait()
    all_but_one(gram_parts, 0, wide_send.at[6]).wait()


def solution(mesh):
    groups = mesh.shape["grp"]
    n = mesh.shape["sub"] * groups
    inner = math.gcd(n, 8)

    def shards(
        rr_inverse,
        corner_modes,
        coarse_inverse,
        inertia,
        disp_now,
        vel_now,
        acc_now,
        load_next,
        basis_rows,
        piece_owner,
    ):
        case_count, sub_count, unknowns = disp_now.shape
        rank = basis_rows.shape[1]
        local_rows = basis_rows.shape[0]
        width = (sub_count + 2) * NC
        f32 = jnp.float32
        vmem = pl.BlockSpec(memory_space=pltpu.VMEM)
        anywhere = pl.BlockSpec(memory_space=pl.ANY)
        results = (
            jax.ShapeDtypeStruct(disp_now.shape, f32),
            jax.ShapeDtypeStruct(disp_now.shape, f32),
            jax.ShapeDtypeStruct((case_count, rank), f32),
            jax.ShapeDtypeStruct((case_count, case_count), f32),
            jax.ShapeDtypeStruct((case_count, local_rows), f32),
        )
        computed = pl.pallas_call(
            functools.partial(kernel, n, groups, inner),
            out_shape=results,
            in_specs=[anywhere] * 10,
            out_specs=(vmem,) * 5,
            scratch_shapes=[
                pltpu.SMEM(piece_owner.shape, jnp.int32),
                pltpu.SMEM(piece_owner.shape, jnp.int32),
                pltpu.VMEM(inertia.shape, f32),
                pltpu.VMEM(disp_now.shape, f32),
                pltpu.VMEM(vel_now.shape, f32),
                pltpu.VMEM(acc_now.shape, f32),
                pltpu.VMEM(load_next.shape, f32),
                pltpu.VMEM((3, width, coarse_inverse.shape[1]), jnp.bfloat16),
                pltpu.VMEM((3, width, sub_count * NI), jnp.bfloat16),
                pltpu.VMEM((3,) + basis_rows.shape, jnp.bfloat16),
                pltpu.VMEM(rr_inverse.shape, f32),
                pltpu.VMEM(corner_modes.shape, f32),
                pltpu.VMEM((width, coarse_inverse.shape[1]), f32),
                pltpu.VMEM(basis_rows.shape, f32),
                pltpu.VMEM((2 * NC, NI), f32),
                pltpu.VMEM((2 * NI, NI), f32),
                pltpu.VMEM((width, sub_count * unknowns), f32),
                pltpu.VMEM((width, sub_count * NI), f32),
                pltpu.VMEM((3, n, case_count, width), f32),
                pltpu.VMEM((5, case_count, NI), f32),
                pltpu.VMEM((5, case_count, NI), f32),
                pltpu.VMEM((1, n, 1, LANES), f32),
                pltpu.VMEM((n, case_count, LANES), f32),
                pltpu.VMEM((n, case_count, LANES), f32),
                pltpu.VMEM((1, n, case_count, LANES), f32),
                pltpu.VMEM((inner, case_count, rank), f32),
                pltpu.VMEM((n // inner, case_count, rank), f32),
                pltpu.VMEM((1, n, 1, LANES), f32),
                pltpu.VMEM((sub_count, case_count, unknowns), f32),
                pltpu.SemaphoreType.DMA((10,)),
                pltpu.SemaphoreType.DMA((5,)),
                pltpu.SemaphoreType.DMA((5,)),
                pltpu.SemaphoreType.DMA((8,)),
                pltpu.SemaphoreType.DMA((8,)),
                pltpu.SemaphoreType.DMA((5,)),
                pltpu.SemaphoreType.DMA((5,)),
            ],
            compiler_params=pltpu.CompilerParams(collective_id=0, has_side_effects=True),
        )(
            piece_owner,
            rr_inverse,
            corner_modes,
            coarse_inverse,
            basis_rows,
            inertia,
            disp_now,
            vel_now,
            acc_now,
            load_next,
        )
        disp, vel, proj, r_factor, columns = pl.pallas_call(
            hand_over, out_shape=results, in_specs=[vmem] * 5, out_specs=(vmem,) * 5
        )(*computed)
        return disp, vel, proj.T, r_factor, columns

    return jax.shard_map(
        shards,
        mesh=mesh,
        in_specs=(
            P(("sub", "grp"), None, None),
            P(("sub", "grp"), None, None),
            P(("sub", "grp"), None),
            P(("sub", "grp"), None),
            P(None, ("sub", "grp"), None),
            P(None, ("sub", "grp"), None),
            P(None, ("sub", "grp"), None),
            P(None, ("sub", "grp"), None),
            P(("sub", "grp"), None),
            P(),
        ),
        out_specs=(
            P(None, ("sub", "grp"), None),
            P(None, ("sub", "grp"), None),
            P(),
            P(),
            P(None, ("sub", "grp")),
        ),
        check_vma=False,
    )
```
